8 devices in a mesh: dp: 2 (over z, y), tp: 4 (over x, core).
Axes of the slice: x: 2, y: 2, z: 1, core: 2. Of those that a mesh axis runs over, the one named last changes fastest.
Arguments:
- hidden: bfloat16 [4096, 2048], P('dp')
- w_final: float32 [2048], replicated
- emb_table: bfloat16 [49152, 2048], P('tp')
- teacher: bfloat16 [4096, 49152], P('dp', 'tp')
- tok_mask: float32 [4096], P('dp')
Outputs:
- output 1: float32 [], replicated
- output 2: bfloat16 [4096, 2048], P('dp')
- output 3: float32 [2048], replicated
- output 4: float32 [49152, 2048], P('tp')
All inputs are finite; a program needn't handle non-finite values.
Results may differ from the reference program's by a relative error of at most 0.00107734.
Values sent between devices are 32-bit elements.
A program may use at most 1 GiB of HBM per device.

```python
import math
import jax
import jax.numpy as jnp
from jax import lax

MODEL_DIM = 2048
VOCAB_SIZE = 49152
NUM_TOKENS = 4096
SEQ_LEN = 16
ROW_BLOCK = math.gcd(NUM_TOKENS, 64)
SOFT_CAP = 30.0
NORM_EPS = 1e-6


def setup_inputs(seed: int = 0) -> dict:
    root_key = jax.random.key(seed)
    k_hid, k_gain, k_dir, k_tab, k_off, k_tea, k_seq, k_tok = jax.random.split(root_key, 8)
    fan_scale = 1.0 / math.sqrt(MODEL_DIM)
    hidden = 3.0 * jax.random.normal(k_hid, (NUM_TOKENS, MODEL_DIM), jnp.float32)
    w_final = 0.3 * jax.random.normal(k_gain, (MODEL_DIM,), jnp.float32)
    direction = 15.0 * fan_scale * jax.random.normal(k_dir, (MODEL_DIM,), jnp.float32)
    emb_table = direction[None, :] + 2.0 * fan_scale * jax.random.normal(k_tab, (VOCAB_SIZE, MODEL_DIM), jnp.float32)
    offset = 15.0 * jax.random.normal(k_off, (NUM_TOKENS, 1), jnp.float32)
    teacher = offset + 3.0 * jax.random.normal(k_tea, (NUM_TOKENS, VOCAB_SIZE), jnp.float32)
    seq_keep = (jax.random.randint(k_seq, (NUM_TOKENS // SEQ_LEN,), 0, 4) > 0).at[0].set(True)
    tok_keep = (jax.random.randint(k_tok, (NUM_TOKENS,), 0, 8) > 0).at[0].set(True)
    tok_mask = jnp.logical_and(jnp.repeat(seq_keep, SEQ_LEN), tok_keep).astype(jnp.float32)
    return {'hidden': hidden.astype(jnp.bfloat16), 'w_final': w_final, 'emb_table': emb_table.astype(jnp.bfloat16), 'teacher': teacher.astype(jnp.bfloat16), 'tok_mask': tok_mask}


def final_norm(hid_rows, w_final):
    hid_f = hid_rows.astype(jnp.float32)
    inv_rms = lax.rsqrt(jnp.mean(hid_f * hid_f, axis=-1, keepdims=True) + NORM_EPS)
    normed = hid_f * inv_rms
    return inv_rms, normed, (normed * (1.0 + w_final)).astype(jnp.bfloat16)


def reference(hidden, w_final, emb_table, teacher, tok_mask):
    mask_sum = jnp.sum(tok_mask)
    num_blocks = NUM_TOKENS // ROW_BLOCK
    hid_blocks = hidden.reshape(num_blocks, ROW_BLOCK, MODEL_DIM)
    tea_blocks = teacher.reshape(num_blocks, ROW_BLOCK, VOCAB_SIZE)
    mask_blocks = tok_mask.reshape(num_blocks, ROW_BLOCK)

    def block_step(scan_carry, block_in):
        loss_acc, gain_acc, table_acc = scan_carry
        hid_rows, tea_rows, mask_rows = block_in
        inv_rms, normed, x_rows = final_norm(hid_rows, w_final)
        logits = jnp.dot(x_rows, emb_table.T, preferred_element_type=jnp.float32)
        stu_cap = SOFT_CAP * jnp.tanh(logits / SOFT_CAP)
        tea_cap = SOFT_CAP * jnp.tanh(tea_rows.astype(jnp.float32) / SOFT_CAP)
        stu_logp = stu_cap - jax.nn.logsumexp(stu_cap, axis=-1, keepdims=True)
        tea_logp = tea_cap - jax.nn.logsumexp(tea_cap, axis=-1, keepdims=True)
        tea_prob = jnp.exp(tea_logp)
        kl_rows = jnp.sum(tea_prob * (tea_logp - stu_logp), axis=-1)
        weight = (mask_rows / mask_sum)[:, None]
        cap_ratio = stu_cap / SOFT_CAP
        grad_z = ((jnp.exp(stu_logp) - tea_prob) * weight * (1.0 - cap_ratio * cap_ratio)).astype(jnp.bfloat16)
        grad_x = jnp.dot(grad_z, emb_table, preferred_element_type=jnp.float32)
        grad_n = grad_x * (1.0 + w_final)
        grad_h = inv_rms * (grad_n - normed * jnp.mean(grad_n * normed, axis=-1, keepdims=True))
        loss_acc = loss_acc + jnp.sum(mask_rows * kl_rows)
        gain_acc = gain_acc + jnp.sum(grad_x * normed, axis=0)
        table_acc = table_acc + jnp.dot(grad_z.T, x_rows, preferred_element_type=jnp.float32)
        return (loss_acc, gain_acc, table_acc), grad_h.astype(jnp.bfloat16)

    init_carry = (jnp.zeros((), jnp.float32), jnp.zeros((MODEL_DIM,), jnp.float32), jnp.zeros((VOCAB_SIZE, MODEL_DIM), jnp.float32))
    (loss_acc, gain_acc, table_acc), grad_blocks = lax.scan(block_step, init_carry, (hid_blocks, tea_blocks, mask_blocks))
    return loss_acc / mask_sum, grad_blocks.reshape(NUM_TOKENS, MODEL_DIM), gain_acc, table_acc
```

```python
import jax
import jax.numpy as jnp
from jax import lax
from jax.sharding import PartitionSpec as P

SOFT_CAP = 30.0
NORM_EPS = 1e-6
TEACHER_CHUNKS = (2048, 2048)
GRAD_CHUNKS = (4096, 3072, 1024)
REST_CHUNKS = (4096, 4096, 3072, 1024)
FIXED = 1024
BUCKETS = (64, 128, 160, 192, 224, 256, 288, 320, 352, 384, 416, 448, 480, 512, 640, 768, 896, 1024)


def final_norm(hid_rows, w_final):
    hid_f = hid_rows.astype(jnp.float32)
    inv_rms = lax.rsqrt(jnp.mean(hid_f * hid_f, axis=-1, keepdims=True) + NORM_EPS)
    normed = hid_f * inv_rms
    return inv_rms, normed, (normed * (1.0 + w_final)).astype(jnp.bfloat16)


def dot_f32(lhs, rhs, dims):
    return lax.dot_general(lhs, rhs, (dims, ((), ())), preferred_element_type=jnp.float32)


def spans(widths, start=0):
    out = []
    for width in widths:
        out.append((start, start + width))
        start += width
    return out


def after(value, *others):
    return lax.optimization_barrier((value, *others))[0]


def solution(mesh):
    n_dp, n_tp = mesh.shape['dp'], mesh.shape['tp']
    swap_dp = [(i, (i + 1) % n_dp) for i in range(n_dp)]
    swap_core = [(i, i ^ 1) for i in range(n_tp)]
    swap_x = [(i, i ^ 2) for i in range(n_tp)]

    def local_step(hid_rows, w_final, tab_rows, tea_rows, mask_rows):
        toks, dim = hid_rows.shape
        me = lax.axis_index('dp')
        tp = lax.axis_index('tp')
        core, xpos = tp % 2, tp // 2

        count = jnp.sum(mask_rows)
        counts = lax.psum(jnp.where(jnp.arange(n_dp) == me, count, 0.0), 'dp')
        counts, mask_rows = lax.optimization_barrier((counts, mask_rows))
        mask_sum = jnp.sum(counts)
        n_other = (mask_sum - count).astype(jnp.int32)
        n_rest = jnp.max(counts).astype(jnp.int32) - FIXED

        iota = jnp.arange(toks, dtype=jnp.int32)
        rank = jnp.sum(jnp.where(iota[None, :] < iota[:, None], mask_rows[None, :], 0.0), axis=1)
        slot = jnp.where(mask_rows > 0.0, rank.astype(jnp.int32), -1)
        pick = (iota[:, None] == slot[None, :]).astype(jnp.bfloat16)
        pick_fixed, pick_rest = pick[:FIXED], pick[FIXED:]
        is_other = jnp.where(iota < n_other, 1.0, 0.0)[:, None]

        inv_rms, normed, x_rows = final_norm(hid_rows, w_final)

        quarter = dim // n_tp
        x_quarter = lax.dynamic_slice_in_dim(x_rows, tp * quarter, quarter, 1)
        x_give = dot_f32(pick, x_quarter, ((1,), (0,)))
        x_part = lax.ppermute(x_give[:FIXED], 'dp', swap_dp)
        x_give_rest = x_give[FIXED:]
        tea_spans = spans(TEACHER_CHUNKS)
        tea_give = []
        for a, b in tea_spans:
            pick_now = after(pick_fixed, *(tea_give or [x_give]))
            tea_give.append(dot_f32(pick_now, tea_rows[:, a:b], ((1,), (0,))))
        tea_got = [lax.ppermute(t, 'dp', swap_dp) for t in tea_give]

        logits = dot_f32(after(x_rows, *tea_give), tab_rows, ((1,), (1,)))
        stu_cap = SOFT_CAP * jnp.tanh(logits / SOFT_CAP)
        tea_cap = SOFT_CAP * jnp.tanh(tea_rows.astype(jnp.float32) / SOFT_CAP)
        stu_exp = jnp.exp(stu_cap - SOFT_CAP)
        tea_exp = jnp.exp(tea_cap - SOFT_CAP)
        part_stats = jnp.stack([jnp.sum(stu_exp, axis=-1), jnp.sum(tea_exp, axis=-1), jnp.sum(tea_exp * (tea_cap - stu_cap), axis=-1)], axis=-1)
        tok_stats = lax.psum(part_stats, 'tp')
        weight = mask_rows / mask_sum
        cap_ratio = stu_cap / SOFT_CAP
        grad_z = ((stu_exp / tok_stats[:, 0:1] - tea_exp / tok_stats[:, 1:2]) * weight[:, None] * (1.0 - cap_ratio * cap_ratio)).astype(jnp.bfloat16)

        pick_idx = jnp.sum(jnp.where(iota[:FIXED, None] == slot[None, :], iota[None, :], 0), axis=1)
        norms = jnp.take(tok_stats[:, :2], pick_idx, axis=0)
        norms_o = lax.ppermute(norms, 'dp', swap_dp)

        grad_spans = spans(GRAD_CHUNKS, tea_spans[-1][1])
        grad_z = after(grad_z, norms)
        grad_give = []
        for a, b in grad_spans:
            pick_now = after(pick_fixed, *grad_give)
            grad_give.append(dot_f32(pick_now, grad_z[:, a:b], ((1,), (0,))))
        grad_got = [lax.ppermute(g, 'dp', swap_dp) for g in grad_give]
        grad_z = after(grad_z, *grad_give)
        rest_spans = spans(REST_CHUNKS)
        rest_give = [dot_f32(pick_rest, grad_z[:, a:b], ((1,), (0,))) for a, b in rest_spans]

        grad_x_part = jnp.dot(grad_z, tab_rows, preferred_element_type=jnp.float32)
        half, quart = toks // 2, toks // 4
        keep = lax.dynamic_slice_in_dim(grad_x_part, core * half, half, 0)
        give = lax.dynamic_slice_in_dim(grad_x_part, (1 - core) * half, half, 0)
        keep = keep + lax.ppermute(give, 'tp', swap_core)
        keep2 = lax.dynamic_slice_in_dim(keep, xpos * quart, quart, 0)
        give2 = lax.dynamic_slice_in_dim(keep, (1 - xpos) * quart, quart, 0)
        grad_x = keep2 + lax.ppermute(give2, 'tp', swap_x)
        norm_q = lax.dynamic_slice_in_dim(normed, core * half + xpos * quart, quart, 0)
        grad_n = grad_x * (1.0 + w_final)
        grad_h = grad_n - norm_q * jnp.mean(grad_n * norm_q, axis=-1, keepdims=True)
        from_x = lax.ppermute(grad_h, 'tp', swap_x)
        rows_half = jnp.where(xpos == 0, jnp.concatenate([grad_h, from_x], 0), jnp.concatenate([from_x, grad_h], 0))
        from_core = lax.ppermute(rows_half, 'tp', swap_core)
        grad_h = jnp.where(core == 0, jnp.concatenate([rows_half, from_core], 0), jnp.concatenate([from_core, rows_half], 0))
        grad_h = (inv_rms * grad_h).astype(jnp.bfloat16)

        kl_rows = tok_stats[:, 2] / tok_stats[:, 1] + jnp.log(tok_stats[:, 0]) - jnp.log(tok_stats[:, 1])
        loss_part = jnp.where(tp == 0, jnp.sum(mask_rows * kl_rows), 0.0)
        gain_part = jnp.sum(grad_x * norm_q, axis=0)
        totals = jnp.concatenate([gain_part, jnp.broadcast_to(loss_part, (dim,))]).reshape(2, dim)
        totals = totals + lax.ppermute(totals, 'tp', swap_core)
        totals = totals + lax.ppermute(totals, 'tp', swap_x)
        totals_o = lax.ppermute(totals, 'dp', swap_dp)

        def join_x(part, valid):
            q_x = lax.ppermute(part, 'tp', swap_x)
            q_mine = jnp.stack([jnp.where(xpos == 0, part, q_x), jnp.where(xpos == 0, q_x, part)])
            q_core = lax.ppermute(q_mine, 'tp', swap_core)
            lo, hi = jnp.where(core == 0, q_mine, q_core), jnp.where(core == 0, q_core, q_mine)
            return (valid * jnp.concatenate([lo[0], hi[0], lo[1], hi[1]], axis=1)).astype(jnp.bfloat16)

        live, live_rest = is_other[:FIXED], is_other[FIXED:]
        x_fixed = join_x(x_part, live)

        grad_table = dot_f32(grad_z, x_rows, ((0,), (0,)))
        for (a, b), tea_c in zip(tea_spans, tea_got):
            ratio = jnp.tanh(dot_f32(x_fixed, tab_rows[a:b], ((1,), (1,))) / SOFT_CAP)
            s_exp = jnp.exp(SOFT_CAP * ratio - SOFT_CAP)
            t_exp = jnp.exp(SOFT_CAP * jnp.tanh(tea_c / SOFT_CAP) - SOFT_CAP)
            norms_o, grad_table = lax.optimization_barrier((norms_o, grad_table))
            g_c = ((s_exp / norms_o[:, 0:1] - t_exp / norms_o[:, 1:2]) * (live / mask_sum) * (1.0 - ratio * ratio)).astype(jnp.bfloat16)
            grad_table = grad_table.at[a:b].add(dot_f32(g_c, x_fixed, ((0,), (0,))))
        grad_table, grad_h, live = lax.optimization_barrier((grad_table, grad_h, live))
        got_fixed = [jnp.zeros((0, tea_spans[-1][1]), jnp.bfloat16)]
        for g in grad_got:
            got_fixed.append((g * live).astype(jnp.bfloat16))
            live = after(live, got_fixed[-1])

        def rest(rows):
            def run(table, x_fixed, x_give, live, fixed, gives):
                live = live[:rows]
                x_part = lax.ppermute(x_give[:rows], 'dp', swap_dp)
                got = [lax.ppermute(g[:rows], 'dp', swap_dp) for g in gives]
                x_rest = join_x(x_part, live)
                x_both = jnp.concatenate([x_fixed, x_rest], 0)
                for (a, b), first, g in zip(rest_spans, fixed, got):
                    g = (g * live).astype(jnp.bfloat16)
                    if first.shape[0]:
                        part = dot_f32(jnp.concatenate([first, g], 0), x_both, ((0,), (0,)))
                    else:
                        part = dot_f32(g, x_rest, ((0,), (0,)))
                    table = table.at[a:b].add(part)
                    live, table = lax.optimization_barrier((live, table))
                return table
            return run

        def only_fixed(table, x_fixed, x_give, live, fixed, gives):
            for (a, b), first in zip(rest_spans[1:], fixed[1:]):
                table = table.at[a:b].add(dot_f32(first, x_fixed, ((0,), (0,))))
            return table

        which = jnp.sum((n_rest > jnp.array((0,) + BUCKETS, jnp.int32)).astype(jnp.int32))
        branches = [only_fixed] + [rest(rows) for rows in BUCKETS]
        grad_table = lax.switch(which, branches, grad_table, x_fixed, x_give_rest, live_rest, got_fixed, rest_give)
        grad_table, totals_o = lax.optimization_barrier((grad_table, totals_o))
        totals = totals + totals_o
        return totals[1, 0] / mask_sum, grad_h, totals[0], grad_table

    return jax.shard_map(local_step, mesh=mesh, in_specs=(P('dp', None), P(None), P('tp', None), P('dp', 'tp'), P('dp')), out_specs=(P(), P('dp', None), P(None), P('tp', None)), check_vma=False)
```

```python
import jax
import jax.numpy as jnp
from jax import lax
from jax.sharding import PartitionSpec as P

SOFT_CAP = 30.0
NORM_EPS = 1e-6
TEACHER_CHUNKS = (2048, 2048)
GRAD_CHUNKS = (5632, 1536, 1024)
REST_CHUNKS = (4096, 5632, 1536, 1024)
FIXED = 1024
BUCKETS = (256, 320, 352, 384, 416, 448, 512, 640, 1024)
GROUP = 3


def final_norm(hid_rows, w_final):
    hid_f = hid_rows.astype(jnp.float32)
    inv_rms = lax.rsqrt(jnp.mean(hid_f * hid_f, axis=-1, keepdims=True) + NORM_EPS)
    normed = hid_f * inv_rms
    return inv_rms, normed, (normed * (1.0 + w_final)).astype(jnp.bfloat16)


def dot_f32(lhs, rhs, dims):
    return lax.dot_general(lhs, rhs, (dims, ((), ())), preferred_element_type=jnp.float32)


def spans(widths, start=0):
    out = []
    for width in widths:
        out.append((start, start + width))
        start += width
    return out


def after(value, *others):
    return lax.optimization_barrier((value, *others))[0]


def solution(mesh):
    n_dp, n_tp = mesh.shape['dp'], mesh.shape['tp']
    swap_dp = [(i, (i + 1) % n_dp) for i in range(n_dp)]
    swap_core = [(i, i ^ 1) for i in range(n_tp)]
    swap_x = [(i, i ^ 2) for i in range(n_tp)]

    def local_step(hid_rows, w_final, tab_rows, tea_rows, mask_rows):
        toks, dim = hid_rows.shape
        tp = lax.axis_index('tp')
        core, xpos = tp % 2, tp // 2

        count = jnp.sum(mask_rows)
        count_o = lax.ppermute(jnp.broadcast_to(count, (8, 128)), 'dp', swap_dp)[0, 0]
        mask_sum = count + count_o
        n_other = count_o.astype(jnp.int32)
        n_rest = jnp.maximum(count, count_o).astype(jnp.int32) - FIXED

        iota = jnp.arange(toks, dtype=jnp.int32)
        rank = jnp.sum(jnp.where(iota[None, :] < iota[:, None], mask_rows[None, :], 0.0), axis=1)
        slot = jnp.where(mask_rows > 0.0, rank.astype(jnp.int32), -1)
        pick = (iota[:, None] == slot[None, :]).astype(jnp.bfloat16)
        pick_fixed, pick_rest = pick[:FIXED], pick[FIXED:]
        is_other = jnp.where(iota < n_other, 1.0, 0.0)[:, None]

        inv_rms, normed, x_rows = final_norm(hid_rows, w_final)

        quarter = dim // n_tp
        x_quarter = lax.dynamic_slice_in_dim(x_rows, tp * quarter, quarter, 1)
        x_give = dot_f32(pick, x_quarter, ((1,), (0,)))
        x_part = lax.ppermute(x_give[:FIXED], 'dp', swap_dp)
        x_give_rest = x_give[FIXED:]
        tea_spans = spans(TEACHER_CHUNKS)
        tea_give = []
        for a, b in tea_spans:
            pick_now = after(pick_fixed, *(tea_give or [x_give]))
            tea_give.append(dot_f32(pick_now, tea_rows[:, a:b], ((1,), (0,))))
        tea_got = [lax.ppermute(t, 'dp', swap_dp) for t in tea_give]

        logits = dot_f32(after(x_rows, x_part, count_o, *tea_give), tab_rows, ((1,), (1,)))
        stu_cap = SOFT_CAP * jnp.tanh(logits / SOFT_CAP)
        tea_cap = SOFT_CAP * jnp.tanh(tea_rows.astype(jnp.float32) / SOFT_CAP)
        stu_exp = jnp.exp(stu_cap - SOFT_CAP)
        tea_exp = jnp.exp(tea_cap - SOFT_CAP)
        part_stats = jnp.stack([jnp.sum(stu_exp, axis=-1), jnp.sum(tea_exp, axis=-1), jnp.sum(tea_exp * (tea_cap - stu_cap), axis=-1)], axis=-1)
        tok_stats = lax.psum(part_stats, 'tp')
        tok_stats, tea_got[0] = lax.optimization_barrier((tok_stats, tea_got[0]))
        weight = mask_rows / mask_sum
        cap_ratio = stu_cap / SOFT_CAP
        grad_z = ((stu_exp / tok_stats[:, 0:1] - tea_exp / tok_stats[:, 1:2]) * weight[:, None] * (1.0 - cap_ratio * cap_ratio)).astype(jnp.bfloat16)

        pick_idx = jnp.sum(jnp.where(iota[:FIXED, None] == slot[None, :], iota[None, :], 0), axis=1)
        norms = jnp.take(tok_stats[:, :2], pick_idx, axis=0)
        norms_o = lax.ppermute(norms, 'dp', swap_dp)

        grad_spans = spans(GRAD_CHUNKS, tea_spans[-1][1])
        grad_z = after(grad_z, norms)
        grad_give = []
        for a, b in grad_spans:
            pick_now = after(pick_fixed, *grad_give)
            grad_give.append(dot_f32(pick_now, grad_z[:, a:b], ((1,), (0,))))
        grad_got = [lax.ppermute(g, 'dp', swap_dp) for g in grad_give]
        grad_z = after(grad_z, *grad_give)
        rest_spans = spans(REST_CHUNKS)
        rest_give = [dot_f32(pick_rest, grad_z[:, a:b], ((1,), (0,))) for a, b in rest_spans]

        grad_z, tea_got[1] = lax.optimization_barrier((grad_z, tea_got[1]))
        grad_x_part = jnp.dot(grad_z, tab_rows, preferred_element_type=jnp.float32)
        half, quart = toks // 2, toks // 4
        keep = lax.dynamic_slice_in_dim(grad_x_part, core * half, half, 0)
        give = lax.dynamic_slice_in_dim(grad_x_part, (1 - core) * half, half, 0)
        keep = keep + lax.ppermute(give, 'tp', swap_core)
        keep2 = lax.dynamic_slice_in_dim(keep, xpos * quart, quart, 0)
        give2 = lax.dynamic_slice_in_dim(keep, (1 - xpos) * quart, quart, 0)
        grad_x = keep2 + lax.ppermute(give2, 'tp', swap_x)
        norm_q = lax.dynamic_slice_in_dim(normed, core * half + xpos * quart, quart, 0)
        grad_n = grad_x * (1.0 + w_final)
        grad_h = grad_n - norm_q * jnp.mean(grad_n * norm_q, axis=-1, keepdims=True)
        from_x = lax.ppermute(grad_h, 'tp', swap_x)
        rows_half = jnp.where(xpos == 0, jnp.concatenate([grad_h, from_x], 0), jnp.concatenate([from_x, grad_h], 0))
        from_core = lax.ppermute(rows_half, 'tp', swap_core)
        grad_h = jnp.where(core == 0, jnp.concatenate([rows_half, from_core], 0), jnp.concatenate([from_core, rows_half], 0))
        grad_h = (inv_rms * grad_h).astype(jnp.bfloat16)

        kl_rows = tok_stats[:, 2] / tok_stats[:, 1] + jnp.log(tok_stats[:, 0]) - jnp.log(tok_stats[:, 1])
        loss_part = jnp.where(tp == 0, jnp.sum(mask_rows * kl_rows), 0.0)
        gain_part = jnp.sum(grad_x * norm_q, axis=0)
        totals = jnp.concatenate([gain_part, jnp.broadcast_to(loss_part, (dim,))]).reshape(2, dim)
        totals = totals + lax.ppermute(totals, 'tp', swap_core)
        totals = totals + lax.ppermute(totals, 'tp', swap_x)
        totals_o = lax.ppermute(totals, 'dp', swap_dp)

        def join_x(part, valid):
            q_x = lax.ppermute(part, 'tp', swap_x)
            q_mine = jnp.stack([jnp.where(xpos == 0, part, q_x), jnp.where(xpos == 0, q_x, part)])
            q_core = lax.ppermute(q_mine, 'tp', swap_core)
            lo, hi = jnp.where(core == 0, q_mine, q_core), jnp.where(core == 0, q_core, q_mine)
            return (valid * jnp.concatenate([lo[0], hi[0], lo[1], hi[1]], axis=1)).astype(jnp.bfloat16)

        live, live_rest = is_other[:FIXED], is_other[FIXED:]
        x_fixed = join_x(x_part, live)

        grad_table = dot_f32(grad_z, x_rows, ((0,), (0,)))
        for (a, b), tea_c in zip(tea_spans, tea_got):
            ratio = jnp.tanh(dot_f32(x_fixed, tab_rows[a:b], ((1,), (1,))) / SOFT_CAP)
            s_exp = jnp.exp(SOFT_CAP * ratio - SOFT_CAP)
            t_exp = jnp.exp(SOFT_CAP * jnp.tanh(tea_c / SOFT_CAP) - SOFT_CAP)
            norms_o, grad_table = lax.optimization_barrier((norms_o, grad_table))
            g_c = ((s_exp / norms_o[:, 0:1] - t_exp / norms_o[:, 1:2]) * (live / mask_sum) * (1.0 - ratio * ratio)).astype(jnp.bfloat16)
            grad_table = grad_table.at[a:b].add(dot_f32(g_c, x_fixed, ((0,), (0,))))
        grad_table, grad_h, live = lax.optimization_barrier((grad_table, grad_h, live))
        got_fixed = [jnp.zeros((0, tea_spans[-1][1]), jnp.bfloat16)]
        for g in grad_got:
            got_fixed.append((g * live).astype(jnp.bfloat16))
            live = after(live, got_fixed[-1])

        def rest(rows):
            def run(table, x_fixed, x_give, live, fixed, gives):
                live = live[:rows]
                x_part = lax.ppermute(x_give[:rows], 'dp', swap_dp)
                got = []
                for i, g in enumerate(gives):
                    if i:
                        g = after(g, x_part if i == 1 else got[i - 2])
                    got.append(lax.ppermute(g[:rows], 'dp', swap_dp))
                x_rest = join_x(x_part, live)
                x_both = jnp.concatenate([x_fixed, x_rest], 0)
                for (a, b), first, g in zip(rest_spans, fixed, got):
                    g = (g * live).astype(jnp.bfloat16)
                    if first.shape[0]:
                        part = dot_f32(jnp.concatenate([first, g], 0), x_both, ((0,), (0,)))
                    else:
                        part = dot_f32(g, x_rest, ((0,), (0,)))
                    table = table.at[a:b].add(part)
                    live, table = lax.optimization_barrier((live, table))
                return table
            return run

        which = jnp.sum((n_rest > jnp.array(BUCKETS[:-1], jnp.int32)).astype(jnp.int32))

        def group(first):
            sizes = BUCKETS[first:first + GROUP]
            return lambda *args: lax.switch(which - first, [rest(rows) for rows in sizes], *args)

        groups = [group(first) for first in range(0, len(BUCKETS), GROUP)]
        grad_table = lax.switch(which // GROUP, groups, grad_table, x_fixed, x_give_rest, live_rest, got_fixed, rest_give)
        grad_table, totals_o = lax.optimization_barrier((grad_table, totals_o))
        totals = totals + totals_o
        return totals[1, 0] / mask_sum, grad_h, totals[0], grad_table

    return jax.shard_map(local_step, mesh=mesh, in_specs=(P('dp', None), P(None), P('tp', None), P('dp', 'tp'), P('dp')), out_specs=(P(), P('dp', None), P(None), P('tp', None)), check_vma=False)
```

```python
import jax
import jax.numpy as jnp
from jax import lax
from jax.sharding import PartitionSpec as P

SOFT_CAP = 30.0
NORM_EPS = 1e-6
TEACHER_CHUNKS = (2048, 2048)
GRAD_CHUNKS = (5632, 1536, 1024)
REST_CHUNKS = (4096, 5632, 1536, 1024)
FIXED = 1024
BUCKETS = (256, 320, 352, 384, 416, 448, 512, 640, 1024)
GROUP = 3


def final_norm(hid_rows, w_final):
    hid_f = hid_rows.astype(jnp.float32)
    inv_rms = lax.rsqrt(jnp.mean(hid_f * hid_f, axis=-1, keepdims=True) + NORM_EPS)
    normed = hid_f * inv_rms
    return inv_rms, normed, (normed * (1.0 + w_final)).astype(jnp.bfloat16)


def dot_f32(lhs, rhs, dims):
    return lax.dot_general(lhs, rhs, (dims, ((), ())), preferred_element_type=jnp.float32)


def spans(widths, start=0):
    out = []
    for width in widths:
        out.append((start, start + width))
        start += width
    return out


def after(value, *others):
    return lax.optimization_barrier((value, *others))[0]


def solution(mesh):
    n_dp, n_tp = mesh.shape['dp'], mesh.shape['tp']
    swap_dp = [(i, (i + 1) % n_dp) for i in range(n_dp)]
    swap_core = [(i, i ^ 1) for i in range(n_tp)]
    swap_x = [(i, i ^ 2) for i in range(n_tp)]

    def local_step(hid_rows, w_final, tab_rows, tea_rows, mask_rows):
        toks, dim = hid_rows.shape
        tp = lax.axis_index('tp')
        core, xpos = tp % 2, tp // 2

        count = jnp.sum(mask_rows)
        count_o = lax.ppermute(jnp.broadcast_to(count, (8, 128)), 'dp', swap_dp)[0, 0]
        mask_sum = count + count_o
        n_other = count_o.astype(jnp.int32)
        n_rest = jnp.maximum(count, count_o).astype(jnp.int32) - FIXED

        iota = jnp.arange(toks, dtype=jnp.int32)
        rank = jnp.sum(jnp.where(iota[None, :] < iota[:, None], mask_rows[None, :], 0.0), axis=1)
        slot = jnp.where(mask_rows > 0.0, rank.astype(jnp.int32), -1)
        pick = (iota[:, None] == slot[None, :]).astype(jnp.bfloat16)
        pick_fixed, pick_rest = pick[:FIXED], pick[FIXED:]
        is_other = jnp.where(iota < n_other, 1.0, 0.0)[:, None]

        inv_rms, normed, x_rows = final_norm(hid_rows, w_final)

        quarter = dim // n_tp
        x_quarter = lax.dynamic_slice_in_dim(x_rows, tp * quarter, quarter, 1)
        x_give = dot_f32(pick, x_quarter, ((1,), (0,)))
        x_part = lax.ppermute(x_give[:FIXED], 'dp', swap_dp)
        x_give_rest = x_give[FIXED:]
        tea_spans = spans(TEACHER_CHUNKS)
        tea_give = []
        for a, b in tea_spans:
            pick_now = after(pick_fixed, *(tea_give or [x_give]))
            tea_give.append(dot_f32(pick_now, tea_rows[:, a:b], ((1,), (0,))))
        tea_got = [lax.ppermute(t, 'dp', swap_dp) for t in tea_give]

        logits = dot_f32(after(x_rows, x_part, count_o, *tea_give), tab_rows, ((1,), (1,)))
        stu_cap = SOFT_CAP * jnp.tanh(logits / SOFT_CAP)
        tea_cap = SOFT_CAP * jnp.tanh(tea_rows.astype(jnp.float32) / SOFT_CAP)
        stu_exp = jnp.exp(stu_cap - SOFT_CAP)
        tea_exp = jnp.exp(tea_cap - SOFT_CAP)
        part_stats = jnp.stack([jnp.sum(stu_exp, axis=-1), jnp.sum(tea_exp, axis=-1), jnp.sum(tea_exp * (tea_cap - stu_cap), axis=-1)], axis=-1)
        tok_stats = lax.psum(part_stats, 'tp')
        tok_stats, tea_got[0] = lax.optimization_barrier((tok_stats, tea_got[0]))
        weight = mask_rows / mask_sum
        cap_ratio = stu_cap / SOFT_CAP
        grad_z = ((stu_exp / tok_stats[:, 0:1] - tea_exp / tok_stats[:, 1:2]) * weight[:, None] * (1.0 - cap_ratio * cap_ratio)).astype(jnp.bfloat16)

        pick_idx = jnp.sum(jnp.where(iota[:FIXED, None] == slot[None, :], iota[None, :], 0), axis=1)
        norms = jnp.take(tok_stats[:, :2], pick_idx, axis=0)
        norms_o = lax.ppermute(norms, 'dp', swap_dp)

        grad_spans = spans(GRAD_CHUNKS, tea_spans[-1][1])
        grad_z = after(grad_z, norms)
        grad_give = []
        for a, b in grad_spans:
            pick_now = after(pick_fixed, *grad_give)
            grad_give.append(dot_f32(pick_now, grad_z[:, a:b], ((1,), (0,))))
        grad_got = [lax.ppermute(g, 'dp', swap_dp) for g in grad_give]
        grad_z = after(grad_z, *grad_give)
        rest_spans = spans(REST_CHUNKS)
        rest_give = [dot_f32(pick_rest, grad_z[:, a:b], ((1,), (0,))) for a, b in rest_spans]

        grad_z, tea_got[1] = lax.optimization_barrier((grad_z, tea_got[1]))
        grad_x_part = jnp.dot(grad_z, tab_rows, preferred_element_type=jnp.float32)
        half, quart = toks // 2, toks // 4
        keep = lax.dynamic_slice_in_dim(grad_x_part, core * half, half, 0)
        give = lax.dynamic_slice_in_dim(grad_x_part, (1 - core) * half, half, 0)
        keep = keep + lax.ppermute(give, 'tp', swap_core)
        keep2 = lax.dynamic_slice_in_dim(keep, xpos * quart, quart, 0)
        give2 = lax.dynamic_slice_in_dim(keep, (1 - xpos) * quart, quart, 0)
        grad_x = keep2 + lax.ppermute(give2, 'tp', swap_x)
        norm_q = lax.dynamic_slice_in_dim(normed, core * half + xpos * quart, quart, 0)
        grad_n = grad_x * (1.0 + w_final)
        grad_h = grad_n - norm_q * jnp.mean(grad_n * norm_q, axis=-1, keepdims=True)
        from_x = lax.ppermute(grad_h, 'tp', swap_x)
        rows_half = jnp.where(xpos == 0, jnp.concatenate([grad_h, from_x], 0), jnp.concatenate([from_x, grad_h], 0))
        from_core = lax.ppermute(rows_half, 'tp', swap_core)
        grad_h = jnp.where(core == 0, jnp.concatenate([rows_half, from_core], 0), jnp.concatenate([from_core, rows_half], 0))
        grad_h = (inv_rms * grad_h).astype(jnp.bfloat16)

        kl_rows = tok_stats[:, 2] / tok_stats[:, 1] + jnp.log(tok_stats[:, 0]) - jnp.log(tok_stats[:, 1])
        loss_part = jnp.where(tp == 0, jnp.sum(mask_rows * kl_rows), 0.0)
        gain_part = jnp.sum(grad_x * norm_q, axis=0)
        totals = jnp.concatenate([gain_part, jnp.broadcast_to(loss_part, (dim,))]).reshape(2, dim)
        totals = totals + lax.ppermute(totals, 'tp', swap_core)
        totals = totals + lax.ppermute(totals, 'tp', swap_x)
        totals_o = lax.ppermute(totals, 'dp', swap_dp)

        def join_x(part, valid):
            q_x = lax.ppermute(part, 'tp', swap_x)
            q_mine = jnp.stack([jnp.where(xpos == 0, part, q_x), jnp.where(xpos == 0, q_x, part)])
            q_core = lax.ppermute(q_mine, 'tp', swap_core)
            lo, hi = jnp.where(core == 0, q_mine, q_core), jnp.where(core == 0, q_core, q_mine)
            return (valid * jnp.concatenate([lo[0], hi[0], lo[1], hi[1]], axis=1)).astype(jnp.bfloat16)

        live, live_rest = is_other[:FIXED], is_other[FIXED:]
        x_fixed = join_x(x_part, live)

        grad_table = dot_f32(grad_z, x_rows, ((0,), (0,)))
        for (a, b), tea_c in zip(tea_spans, tea_got):
            ratio = jnp.tanh(dot_f32(x_fixed, tab_rows[a:b], ((1,), (1,))) / SOFT_CAP)
            s_exp = jnp.exp(SOFT_CAP * ratio - SOFT_CAP)
            t_exp = jnp.exp(SOFT_CAP * jnp.tanh(tea_c / SOFT_CAP) - SOFT_CAP)
            norms_o, grad_table = lax.optimization_barrier((norms_o, grad_table))
            g_c = ((s_exp / norms_o[:, 0:1] - t_exp / norms_o[:, 1:2]) * (live / mask_sum) * (1.0 - ratio * ratio)).astype(jnp.bfloat16)
            grad_table = grad_table.at[a:b].add(dot_f32(g_c, x_fixed, ((0,), (0,))))
        grad_table, grad_h, live = lax.optimization_barrier((grad_table, grad_h, live))
        got_fixed = [jnp.zeros((0, tea_spans[-1][1]), jnp.bfloat16)]
        got_fixed.extend(grad_got)

        def rest(rows):
            def run(table, x_fixed, x_give, live, live_fixed, fixed, gives):
                live = live[:rows]
                x_part = lax.ppermute(x_give[:rows], 'dp', swap_dp)
                got = []
                for i, g in enumerate(gives):
                    if i:
                        g = after(g, x_part if i == 1 else got[i - 2])
                    got.append(lax.ppermute(g[:rows], 'dp', swap_dp))
                x_rest = join_x(x_part, live)
                x_both = jnp.concatenate([x_fixed, x_rest], 0)
                for (a, b), first, g in zip(rest_spans, fixed, got):
                    g = (g * live).astype(jnp.bfloat16)
                    if first.dtype != g.dtype:
                        first = (first * live_fixed).astype(g.dtype)
                    if first.shape[0]:
                        part = dot_f32(jnp.concatenate([first, g], 0), x_both, ((0,), (0,)))
                    else:
                        part = dot_f32(g, x_rest, ((0,), (0,)))
                    table = table.at[a:b].add(part)
                    live, table = lax.optimization_barrier((live, table))
                return table
            return run

        which = jnp.sum((n_rest > jnp.array(BUCKETS[:-1], jnp.int32)).astype(jnp.int32))

        def group(first):
            sizes = BUCKETS[first:first + GROUP]
            return lambda *args: lax.switch(which - first, [rest(rows) for rows in sizes], *args)

        groups = [group(first) for first in range(0, len(BUCKETS), GROUP)]
        grad_table = lax.switch(which // GROUP, groups, grad_table, x_fixed, x_give_rest, live_rest, live, got_fixed, rest_give)
        grad_table, totals_o = lax.optimization_barrier((grad_table, totals_o))
        totals = totals + totals_o
        return totals[1, 0] / mask_sum, grad_h, totals[0], grad_table

    return jax.shard_map(local_step, mesh=mesh, in_specs=(P('dp', None), P(None), P('tp', None), P('dp', 'tp'), P('dp')), out_specs=(P(), P('dp', None), P(None), P('tp', None)), check_vma=False)
```
